64 devices in a mesh: dp: 4 (over x, y), tp: 16 (over z, core).
Axes of the slice: x: 2, y: 2, z: 8, core: 2. Of those that a mesh axis runs over, the one named last changes fastest.
The devices are a block of a 4x4x8 slice.
Arguments:
- ids: int32 [32, 256], P('dp'), parts along dimension 0
- E: bfloat16 [8192, 4096], P('tp')
- g: bfloat16 [4096], replicated
- W: bfloat16 [4096, 6144], P(None, 'tp')
- du: bfloat16 [32, 256, 6144], P('dp', None, 'tp'), parts along dimension 0
- dres: bfloat16 [32, 256, 4096], P('dp', 'tp'), parts along dimension 0
Outputs:
- output 1: bfloat16 [32, 256, 6144], P('dp', None, 'tp'), parts along dimension 0
- output 2: bfloat16 [32, 256, 4096], P('dp', 'tp'), parts along dimension 0
- output 3: float32 [32768, 4096], P(('dp', 'tp')), parts along dimension 0
- output 4: float32 [16384, 6144], P('dp', 'tp'), parts along dimension 0
- output 5: float32 [16384], P('dp'), parts along dimension 0
There are 4 independent parts. The reference program is written for one: setup_inputs(seed, part) draws one part's arguments, and reference() takes and returns one part's arrays. A program takes and returns all parts, laid end to end along the dimension named above; an argument that names none is the same for every part.
All inputs are finite; a program needn't handle non-finite values.
Results may differ from the reference program's by a relative error of at most 0.00672465.
Values are sent between devices in bfloat16 or wider.
A program may use at most 768 MiB of HBM per device.

```python
import jax
import jax.numpy as jnp
from jax import lax

V = 8192
K = 8
T = 256
D = 4096
FC = 6144
TP = 16
NPOP = 256
EPS = 1e-6


def setup_inputs(seed: int = 0, part: int = 0) -> dict:
    key = jax.random.key(seed)
    kp = jax.random.fold_in(key, part)
    k1, k2, k3, k4, k5, k6 = jax.random.split(kp, 6)
    s1, s2, s3 = jax.random.split(key, 3)
    kd = jax.random.fold_in(kp, 7)
    d1, d2, d3, d4 = jax.random.split(kd, 4)
    vs = V // TP
    pop = jnp.arange(TP, dtype=jnp.int32) * vs + jax.random.randint(d1, (TP,), 0, vs, dtype=jnp.int32)
    pick = jax.random.randint(d2, (K, T), 0, TP, dtype=jnp.int32)
    uni = jax.random.randint(d3, (K, T), 0, V, dtype=jnp.int32)
    coin = jax.random.bernoulli(d4, 0.75, (K, T))
    ids = jnp.where(coin, pop[pick], uni).astype(jnp.int32)
    E = jax.random.normal(s1, (V, D), jnp.float32).astype(jnp.bfloat16)
    g = (1.0 + 0.4 * jax.random.normal(s2, (D,), jnp.float32)).astype(jnp.bfloat16)
    W = (jax.random.normal(s3, (D, FC), jnp.float32) * D ** -0.5).astype(jnp.bfloat16)
    du = jax.random.normal(k5, (K, T, FC), jnp.float32).astype(jnp.bfloat16)
    dres = jax.random.normal(k6, (K, T, D), jnp.float32).astype(jnp.bfloat16)
    return {"ids": ids, "E": E, "g": g, "W": W, "du": du, "dres": dres}


def reference(ids, E, g, W, du, dres):
    gf = g.astype(jnp.float32)
    fs = FC // TP
    wr = W.reshape(D, TP, fs).transpose(1, 0, 2)

    def micro(carry, inp):
        dE, dW, dg = carry
        idk, duk, dresk = inp
        x = jnp.take(E, idk, axis=0)
        xf = x.astype(jnp.float32)
        rs = lax.rsqrt(jnp.mean(xf * xf, axis=-1, keepdims=True) + EPS)
        nh = xf * rs
        n = (nh * gf).astype(jnp.bfloat16)
        u = jnp.dot(n, W, preferred_element_type=jnp.float32).astype(jnp.bfloat16)
        dur = duk.reshape(T, TP, fs).transpose(1, 0, 2)

        def add_block(acc, blk):
            dub, wb = blk
            pr = jnp.dot(dub, wb.T, preferred_element_type=jnp.float32)
            return acc + pr.astype(jnp.bfloat16).astype(jnp.float32), None

        dn, _ = lax.scan(add_block, jnp.zeros((T, D), jnp.float32), (dur, wr))
        gdn = gf * dn
        dx = dresk.astype(jnp.float32) + rs * (gdn - nh * jnp.mean(nh * gdn, axis=-1, keepdims=True))
        dxb = dx.astype(jnp.bfloat16).astype(jnp.float32)
        dE = dE.at[idk].add(dxb)
        dW = dW + jnp.dot(n.T, duk, preferred_element_type=jnp.float32)
        dg = dg + jnp.sum(dn * nh, axis=0)
        return (dE, dW, dg), (u, x)

    init = (jnp.zeros((V, D), jnp.float32), jnp.zeros((D, FC), jnp.float32), jnp.zeros((D,), jnp.float32))
    (dE, dW, dg), (u, x) = lax.scan(micro, init, (ids, du, dres))
    return u, x, dE, dW, dg
```

```python
import jax
import jax.numpy as jnp
from jax import lax
from jax.sharding import PartitionSpec as P

EPS = 1e-6
ROWS = 64
LOW = 64


def solution(mesh):
    ntp = mesh.shape["tp"]
    axes = tuple(mesh.axis_names)

    def body(ids, E, g, W, du, dres):
        f32, bf16, i32 = jnp.float32, jnp.bfloat16, jnp.int32
        vs, d = E.shape
        nk, t = ids.shape
        ts = t // ntp
        nt = nk * t
        own = nk * ts
        hn = ntp * vs // LOW
        hs = vs // LOW
        me = lax.axis_index("tp")
        lo = me * vs
        gf = g.astype(f32)
        c0 = (((0,), (0,)), ((), ()))
        c1 = (((1,), (1,)), ((), ()))

        def dot(a, b, c=(((1,), (0,)), ((), ()))):
            return lax.dot_general(a, b, c, preferred_element_type=f32)

        def iota(shape, dim):
            return lax.broadcasted_iota(i32, shape, dim)

        def norm(v):
            vf = v.astype(f32)
            rs = lax.rsqrt(jnp.mean(vf * vf, axis=-1, keepdims=True) + EPS)
            return rs, vf * rs

        idp = ids.reshape(nk, ntp, ts).transpose(1, 0, 2).reshape(nt)
        dup = du.reshape(nk, ntp, ts, -1).transpose(1, 0, 2, 3).reshape(nt, -1)
        dr = dres.reshape(own, d).astype(f32)

        isl = iota((LOW, nt), 0) == (idp % LOW)[None, :]
        ish = iota((hn, nt), 0) == (idp // LOW)[None, :]
        pres = dot(ish.astype(bf16), isl.astype(bf16), c1) > 0
        upper = (iota((LOW, LOW), 0) < iota((LOW, LOW), 1)).astype(bf16)
        inrow = dot(pres.astype(bf16), upper)
        tot = jnp.sum(pres.astype(f32), axis=1)
        ha, hb = iota((hn, hn), 0), iota((hn, hn), 1)
        off = jnp.sum(jnp.where((ha // hs == hb // hs) & (hb < ha), tot[None, :], 0.0), axis=1)
        rank = jnp.where(pres, inrow + off[:, None], -1.0)
        over = jnp.max(rank) >= ROWS
        trank = dot(inrow.astype(bf16), isl.astype(bf16)) + off[:, None]
        trank = jnp.sum(jnp.where(ish, trank, 0.0), axis=0).astype(i32)
        mrank = lax.dynamic_slice_in_dim(rank, me * hs, hs, 0).reshape(vs).astype(i32)

        sel = (iota((ROWS, vs), 0) == mrank[None, :]).astype(bf16)
        xg = lax.all_gather(dot(sel, E).astype(bf16), "tp", axis=0, tiled=True)

        p = lax.reduce_precision(dot(dup, W, c1), 8, 7)
        dn = lax.psum_scatter(p, "tp", scatter_dimension=0, tiled=True)

        q = jnp.where(trank < ROWS, (idp // vs) * ROWS + trank, -1)
        oh = (iota((nt, ntp * ROWS), 1) == q[:, None]).astype(bf16)
        nd = (norm(xg)[1] * gf).astype(bf16)
        n = dot(oh, nd).astype(bf16)
        qo = lax.dynamic_slice_in_dim(q, me * own, own, 0)
        oho = (iota((own, ntp * ROWS), 1) == qo[:, None]).astype(bf16)
        xo = dot(oho, xg).astype(bf16)

        def rest(n, xo, dn, *held):
            u = dot(n, W).astype(bf16)
            dW = dot(n, dup, c0)
            dn, u, dW, *held = lax.optimization_barrier((dn, u, dW) + held)
            rs, nh = norm(xo)
            gdn = gf * dn
            dx = dr + rs * (gdn - nh * jnp.mean(nh * gdn, axis=-1, keepdims=True))
            dxa = lax.all_gather(dx.astype(bf16), "tp", axis=0, tiled=True)
            dg = lax.psum(jnp.sum(dn * nh, axis=0), "tp")
            oht = (iota((vs, nt), 0) == (idp - lo)[None, :]).astype(bf16)
            dE = dot(oht, dxa)
            un = u.reshape(ntp, nk, ts, -1).transpose(1, 0, 2, 3).reshape(nk, t, -1)
            return (*held, un, xo.reshape(nk, ts, d), dE, dW, dg)

        over, n = lax.optimization_barrier((over, n))
        over = lax.pmax(over.astype(i32), axes)
        outs = rest(n, xo, dn, over)

        def slow(c):
            oh = (iota((vs, nt), 0) == (idp - lo)[None, :]).astype(bf16)
            x = lax.psum(dot(oh, E, c0).astype(bf16), "tp")
            n = (norm(x)[1] * gf).astype(bf16)
            return (jnp.int32(0),) + rest(n, lax.dynamic_slice_in_dim(x, me * own, own, 0), dn)

        return lax.while_loop(lambda c: c[0] > 0, slow, outs)[1:]

    return jax.shard_map(
        body,
        mesh=mesh,
        in_specs=(P("dp", None), P("tp", None), P(None), P(None, "tp"), P("dp", None, "tp"), P("dp", "tp", None)),
        out_specs=(P("dp", None, "tp"), P("dp", "tp", None), P(("dp", "tp"), None), P("dp", "tp"), P("dp")),
        check_vma=False,
    )
```

```python
import jax
import jax.numpy as jnp
from jax import lax
from jax.sharding import PartitionSpec as P

EPS = 1e-6
ROWS = 64
LOW = 64


def solution(mesh):
    ntp = mesh.shape["tp"]

    def body(ids, E, g, W, du, dres):
        f32, bf16, i32 = jnp.float32, jnp.bfloat16, jnp.int32
        vs, d = E.shape
        nk, t = ids.shape
        ts = t // ntp
        nt = nk * t
        own = nk * ts
        hn = ntp * vs // LOW
        hs = vs // LOW
        me = lax.axis_index("tp")
        lo = me * vs
        gf = g.astype(f32)
        c0 = (((0,), (0,)), ((), ()))
        c1 = (((1,), (1,)), ((), ()))

        def dot(a, b, c=(((1,), (0,)), ((), ()))):
            return lax.dot_general(a, b, c, preferred_element_type=f32)

        def iota(shape, dim):
            return lax.broadcasted_iota(i32, shape, dim)

        def norm(v):
            vf = v.astype(f32)
            rs = lax.rsqrt(jnp.mean(vf * vf, axis=-1, keepdims=True) + EPS)
            return rs, vf * rs

        idp = ids.reshape(nk, ntp, ts).transpose(1, 0, 2).reshape(nt)
        dup = du.reshape(nk, ntp, ts, -1).transpose(1, 0, 2, 3).reshape(nt, -1)

        isl = iota((LOW, nt), 0) == (idp % LOW)[None, :]
        ish = iota((hn, nt), 0) == (idp // LOW)[None, :]
        pres = dot(ish.astype(bf16), isl.astype(bf16), c1) > 0
        upper = (iota((LOW, LOW), 0) < iota((LOW, LOW), 1)).astype(bf16)
        inrow = dot(pres.astype(bf16), upper)
        tot = jnp.sum(pres.astype(f32), axis=1)
        ha, hb = iota((hn, hn), 0), iota((hn, hn), 1)
        off = jnp.sum(jnp.where((ha // hs == hb // hs) & (hb < ha), tot[None, :], 0.0), axis=1)
        rank = jnp.where(pres, inrow + off[:, None], -1.0)
        over = jnp.max(rank) >= ROWS
        trank = dot(inrow.astype(bf16), isl.astype(bf16)) + off[:, None]
        trank = jnp.sum(jnp.where(ish, trank, 0.0), axis=0).astype(i32)
        mrank = lax.dynamic_slice_in_dim(rank, me * hs, hs, 0).reshape(vs).astype(i32)

        sel = (iota((ROWS, vs), 0) == mrank[None, :]).astype(bf16)
        xg = lax.all_gather(dot(sel, E).astype(bf16), "tp", axis=0, tiled=True)

        dc = d // ntp

        def first(W, dup, dres):
            pT = lax.optimization_barrier(lax.reduce_precision(dot(W, dup, c1), 8, 7))
            dnT = lax.psum_scatter(pT, "tp", scatter_dimension=0, tiled=True)
            dresT = lax.all_to_all(dres.reshape(own, d), "tp", 1, 0, tiled=True).T
            return pT, dnT, dresT

        pT, dnT, dresT = first(W, dup, dres)
        over = lax.pmax(over.astype(i32), "dp")

        q = jnp.where(trank < ROWS, (idp // vs) * ROWS + trank, -1)
        oh = (iota((nt, ntp * ROWS), 1) == q[:, None]).astype(bf16)
        ohT = iota((ntp * ROWS, nt), 0) == q[None, :]
        rst = jnp.sum(jnp.where(ohT, norm(xg)[0], 0.0), axis=0)
        xT = lax.dot_general(xg, oh, (((0,), (1,)), ((), ())), preferred_element_type=f32).astype(bf16)
        qo = lax.dynamic_slice_in_dim(q, me * own, own, 0)
        oho = (iota((own, ntp * ROWS), 1) == qo[:, None]).astype(bf16)
        xo = dot(oho, xg).astype(bf16)

        def ahead(xT, rst, pT, W, dup):
            nhg = xT.astype(f32) * rst[None, :] * gf[:, None]
            mp = jnp.sum(nhg * pT, axis=0)
            nT = nhg.astype(bf16)
            u = dot(nT, W, c0).astype(bf16)
            dW = dot(nT, dup)
            un = u.reshape(ntp, nk, ts, -1).transpose(1, 0, 2, 3).reshape(nk, t, -1)
            return lax.psum(mp, "tp") * (1.0 / d), un, dW

        def behind(xT, rst, m, dnT, dresT):
            nh = lax.dynamic_slice_in_dim(xT, me * dc, dc, 0).astype(f32) * rst[None, :]
            gdn = lax.dynamic_slice_in_dim(gf, me * dc, dc, 0)[:, None] * dnT
            dx = dresT.astype(f32) + rst[None, :] * (gdn - nh * m[None, :])
            return dx.astype(bf16), jnp.sum(dnT * nh, axis=1)

        m, un, dW = ahead(xT, rst, pT, W, dup)
        dnT, m, un, dW, over = lax.optimization_barrier((dnT, m, un, dW, over))
        dxT, dgs = behind(xT, rst, m, dnT, dresT)
        dEc = lax.dot_general(oh, dxT, (((0,), (1,)), ((), ())), preferred_element_type=f32)
        dgr = jnp.broadcast_to(dgs[None, None, :], (ntp, 8, dc))
        got = lax.all_to_all(jnp.concatenate([dEc.reshape(ntp, ROWS, dc), dgr], axis=1), "tp", 0, 0, tiled=True)
        dg = got[:, ROWS, :].reshape(d)
        rows = got[:, :ROWS, :].transpose(1, 0, 2).reshape(ROWS, d)
        put = (iota((vs, ROWS), 1) == mrank[:, None]).astype(f32)
        dE = jnp.dot(put, rows, precision=lax.Precision.HIGHEST, preferred_element_type=f32)
        outs = (over, un, xo.reshape(nk, ts, d), dE, dW, dg)

        def slow(c, ops=(E, W, dup, dres, idp)):
            (E, W, dup, dres, idp), _ = lax.optimization_barrier((ops, c[0]))
            pT, dnT, dresT = first(W, dup, dres)
            oht = (iota((vs, nt), 0) == (idp - lo)[None, :]).astype(bf16)
            x = lax.psum(dot(oht, E, c0).astype(bf16), "tp")
            rst = norm(x)[0][:, 0]
            m, un, dW = ahead(x.T, rst, pT, W, dup)
            dxT, dgs = behind(x.T, rst, m, dnT, dresT)
            dE = dot(oht, lax.all_gather(dxT, "tp", axis=0, tiled=True), c1)
            xo = lax.dynamic_slice_in_dim(x, me * own, own, 0)
            return jnp.int32(0), un, xo.reshape(nk, ts, d), dE, dW, lax.all_gather(dgs, "tp", axis=0, tiled=True)

        return lax.while_loop(lambda c: c[0] > 0, slow, outs)[1:]

    return jax.shard_map(
        body,
        mesh=mesh,
        in_specs=(P("dp", None), P("tp", None), P(None), P(None, "tp"), P("dp", None, "tp"), P("dp", "tp", None)),
        out_specs=(P("dp", None, "tp"), P("dp", "tp", None), P(("dp", "tp"), None), P("dp", "tp"), P("dp")),
        check_vma=False,
    )
```

```python
import jax
import jax.numpy as jnp
from jax import lax
from jax.sharding import PartitionSpec as P

EPS = 1e-6
ROWS = 64
LOW = 64


def solution(mesh):
    ntp = mesh.shape["tp"]

    def body(ids, E, g, W, du, dres):
        f32, bf16, i32 = jnp.float32, jnp.bfloat16, jnp.int32
        vs, d = E.shape
        nk, t = ids.shape
        ts = t // ntp
        nt = nk * t
        own = nk * ts
        hn = ntp * vs // LOW
        hs = vs // LOW
        me = lax.axis_index("tp")
        lo = me * vs
        gf = g.astype(f32)
        c0 = (((0,), (0,)), ((), ()))
        c1 = (((1,), (1,)), ((), ()))

        def dot(a, b, c=(((1,), (0,)), ((), ()))):
            return lax.dot_general(a, b, c, preferred_element_type=f32)

        def iota(shape, dim):
            return lax.broadcasted_iota(i32, shape, dim)

        def norm(v):
            vf = v.astype(f32)
            rs = lax.rsqrt(jnp.mean(vf * vf, axis=-1, keepdims=True) + EPS)
            return rs, vf * rs

        idp = ids.reshape(nk, ntp, ts).transpose(1, 0, 2).reshape(nt)
        dup = du.reshape(nk, ntp, ts, -1).transpose(1, 0, 2, 3).reshape(nt, -1)

        isl = iota((LOW, nt), 0) == (idp % LOW)[None, :]
        ish = iota((hn, nt), 0) == (idp // LOW)[None, :]
        pres = dot(ish.astype(bf16), isl.astype(bf16), c1) > 0
        upper = (iota((LOW, LOW), 0) < iota((LOW, LOW), 1)).astype(bf16)
        inrow = dot(pres.astype(bf16), upper)
        tot = jnp.sum(pres.astype(f32), axis=1)
        ha, hb = iota((hn, hn), 0), iota((hn, hn), 1)
        off = jnp.sum(jnp.where((ha // hs == hb // hs) & (hb < ha), tot[None, :], 0.0), axis=1)
        rank = jnp.where(pres, inrow + off[:, None], -1.0)
        over = jnp.max(rank) >= ROWS
        trank = dot(inrow.astype(bf16), isl.astype(bf16)) + off[:, None]
        trank = jnp.sum(jnp.where(ish, trank, 0.0), axis=0).astype(i32)
        mrank = lax.dynamic_slice_in_dim(rank, me * hs, hs, 0).reshape(vs).astype(i32)

        sel = (iota((ROWS, vs), 0) == mrank[None, :]).astype(bf16)
        xg = lax.all_gather(dot(sel, E).astype(bf16), "tp", axis=0, tiled=True)

        half, dc, npair = d // 2, d // ntp, ntp // 2
        side = me % 2
        swap = [(i, i ^ 1) for i in range(ntp)]
        rows = [list(range(c, ntp, 2)) for c in range(2)]
        start = side * half + (me // 2) * dc

        def rounded(a, b):
            return lax.reduce_precision(dot(a, b, c1), 8, 7)

        def first(W, dup, dres):
            Wo = lax.ppermute(lax.dynamic_slice_in_dim(W, (1 - side) * half, half, 0), "tp", swap)
            duo = lax.ppermute(dup, "tp", swap)
            dr = dres.reshape(own, 2, npair, dc).transpose(0, 2, 1, 3).reshape(own, d)
            dresT = lax.all_to_all(dr, "tp", 1, 0, tiled=True).T
            dup, duo, Wo, dresT = lax.optimization_barrier((dup, duo, Wo, dresT))
            pT = rounded(Wo, duo) + rounded(lax.dynamic_slice_in_dim(W, side * half, half, 0), dup)
            pT = lax.optimization_barrier(pT)
            dnT = lax.psum_scatter(pT, "tp", scatter_dimension=0, axis_index_groups=rows, tiled=True)
            return pT, dnT, dresT

        pT, dnT, dresT = first(W, dup, dres)
        over = lax.pmax(over.astype(i32), "dp")

        q = jnp.where(trank < ROWS, (idp // vs) * ROWS + trank, -1)
        oh = (iota((nt, ntp * ROWS), 1) == q[:, None]).astype(bf16)
        ohT = iota((ntp * ROWS, nt), 0) == q[None, :]
        rst = jnp.sum(jnp.where(ohT, norm(xg)[0], 0.0), axis=0)
        xT = lax.dot_general(xg, oh, (((0,), (1,)), ((), ())), preferred_element_type=f32).astype(bf16)
        qo = lax.dynamic_slice_in_dim(q, me * own, own, 0)
        oho = (iota((own, ntp * ROWS), 1) == qo[:, None]).astype(bf16)
        xo = dot(oho, xg).astype(bf16)

        def ahead(xT, rst, pT, W, dup):
            nh = lax.dynamic_slice_in_dim(xT, side * half, half, 0).astype(f32) * rst[None, :]
            gh = lax.dynamic_slice_in_dim(gf, side * half, half, 0)
            mp = jnp.sum(nh * gh[:, None] * pT, axis=0)
            dgp = jnp.sum(nh * pT, axis=1)
            dgp = jnp.concatenate([jnp.where(side == 0, dgp, 0.0), jnp.where(side == 1, dgp, 0.0)])
            nT = (xT.astype(f32) * rst[None, :] * gf[:, None]).astype(bf16)
            u = dot(nT, W, c0).astype(bf16)
            dW = dot(nT, dup)
            un = u.reshape(ntp, nk, ts, -1).transpose(1, 0, 2, 3).reshape(nk, t, -1)
            both = lax.psum(jnp.concatenate([mp, dgp]), "tp")
            return both[:nt] * (1.0 / d), both[nt:], un, dW

        def behind(xT, rst, m, dnT, dresT):
            nh = lax.dynamic_slice_in_dim(xT, start, dc, 0).astype(f32) * rst[None, :]
            gdn = lax.dynamic_slice_in_dim(gf, start, dc, 0)[:, None] * dnT
            dx = dresT.astype(f32) + rst[None, :] * (gdn - nh * m[None, :])
            return dx.astype(bf16)

        def columns(v):
            return v.reshape(npair, 2, -1, dc).transpose(2, 1, 0, 3).reshape(-1, d)

        m, dg, un, dW = ahead(xT, rst, pT, W, dup)
        dnT, m, dg, un, dW, xo, over = lax.optimization_barrier((dnT, m, dg, un, dW, xo, over))
        dxT = behind(xT, rst, m, dnT, dresT)
        dEc = lax.dot_general(oh, dxT, (((0,), (1,)), ((), ())), preferred_element_type=f32)
        got = lax.all_to_all(dEc.reshape(ntp, ROWS, dc), "tp", 0, 0, tiled=True)
        put = (iota((vs, ROWS), 1) == mrank[:, None]).astype(f32)
        dE = jnp.dot(put, columns(got), precision=lax.Precision.HIGHEST, preferred_element_type=f32)
        outs = (over, un, xo.reshape(nk, ts, d), dE, dW, dg)

        def slow(c, ops=(E, W, dup, dres, idp)):
            (E, W, dup, dres, idp), _ = lax.optimization_barrier((ops, c[0]))
            pT, dnT, dresT = first(W, dup, dres)
            oht = (iota((vs, nt), 0) == (idp - lo)[None, :]).astype(bf16)
            x = lax.psum(dot(oht, E, c0).astype(bf16), "tp")
            rst = norm(x)[0][:, 0]
            m, dg, un, dW = ahead(x.T, rst, pT, W, dup)
            dx = lax.all_gather(behind(x.T, rst, m, dnT, dresT).T, "tp", axis=0, tiled=True)
            dE = dot(oht, columns(dx))
            xo = lax.dynamic_slice_in_dim(x, me * own, own, 0)
            return jnp.int32(0), un, xo.reshape(nk, ts, d), dE, dW, dg

        return lax.while_loop(lambda c: c[0] > 0, slow, outs)[1:]

    return jax.shard_map(
        body,
        mesh=mesh,
        in_specs=(P("dp", None), P("tp", None), P(None), P(None, "tp"), P("dp", None, "tp"), P("dp", "tp", None)),
        out_specs=(P("dp", None, "tp"), P("dp", "tp", None), P(("dp", "tp"), None), P("dp", "tp"), P("dp")),
        check_vma=False,
    )
```

```python
import jax
import jax.numpy as jnp
from jax import lax
from jax.experimental.layout import Layout, with_layout_constraint
from jax.sharding import PartitionSpec as P

EPS = 1e-6
PARTS = 8
PARTS_P = 8
PARTS_R = 8
ROWS = 64
LOW = 64


def solution(mesh):
    ntp = mesh.shape["tp"]

    def body(ids, E, g, W, du, dres):
        f32, bf16, i32 = jnp.float32, jnp.bfloat16, jnp.int32
        vs, d = E.shape
        nk, t = ids.shape
        ts = t // ntp
        nt = nk * t
        own = nk * ts
        hn = ntp * vs // LOW
        hs = vs // LOW
        me = lax.axis_index("tp")
        lo = me * vs
        gf = g.astype(f32)
        c0 = (((0,), (0,)), ((), ()))
        c1 = (((1,), (1,)), ((), ()))

        def dot(a, b, c=(((1,), (0,)), ((), ()))):
            return lax.dot_general(a, b, c, preferred_element_type=f32)

        def iota(shape, dim):
            return lax.broadcasted_iota(i32, shape, dim)

        def plain(v):
            return with_layout_constraint(v, Layout((0, 1)))

        def norm(v):
            vf = v.astype(f32)
            rs = lax.rsqrt(jnp.mean(vf * vf, axis=-1, keepdims=True) + EPS)
            return rs, vf * rs

        idp = ids.reshape(nk, ntp, ts).transpose(1, 0, 2).reshape(nt)
        dup = du.reshape(nk, ntp, ts, -1).transpose(1, 0, 2, 3).reshape(nt, -1)

        isl = iota((LOW, nt), 0) == (idp % LOW)[None, :]
        ish = iota((hn, nt), 0) == (idp // LOW)[None, :]
        pres = dot(ish.astype(bf16), isl.astype(bf16), c1) > 0
        upper = (iota((LOW, LOW), 0) < iota((LOW, LOW), 1)).astype(bf16)
        inrow = dot(pres.astype(bf16), upper)
        tot = jnp.sum(pres.astype(f32), axis=1)
        ha, hb = iota((hn, hn), 0), iota((hn, hn), 1)
        off = jnp.sum(jnp.where((ha // hs == hb // hs) & (hb < ha), tot[None, :], 0.0), axis=1)
        rank = jnp.where(pres, inrow + off[:, None], -1.0)
        over = jnp.max(rank) >= ROWS
        trank = dot(inrow.astype(bf16), isl.astype(bf16)) + off[:, None]
        trank = jnp.sum(jnp.where(ish, trank, 0.0), axis=0).astype(i32)
        mrank = lax.dynamic_slice_in_dim(rank, me * hs, hs, 0).reshape(vs).astype(i32)

        sel = (iota((ROWS, vs), 0) == mrank[None, :]).astype(bf16)
        xg = lax.all_gather(dot(sel, E).astype(bf16), "tp", axis=0, tiled=True)

        half, dc, npair = d // 2, d // ntp, ntp // 2
        side = me % 2
        swap = [(i, i ^ 1) for i in range(ntp)]
        rows = [list(range(c, ntp, 2)) for c in range(2)]
        start = side * half + (me // 2) * dc

        def rounded(a, b):
            return lax.reduce_precision(dot(a, b, c1), 8, 7)

        def first(W, dup, dres):
            Wo = lax.ppermute(lax.dynamic_slice_in_dim(W, (1 - side) * half, half, 0), "tp", swap)
            duo = lax.ppermute(dup, "tp", swap)
            dr = dres.reshape(own, 2, npair, dc).transpose(0, 2, 1, 3).reshape(own, d)
            dresT = lax.all_to_all(dr, "tp", 1, 0, tiled=True)
            dresT = plain(dresT.T)
            dup, duo, Wo, dresT = lax.optimization_barrier((dup, duo, Wo, dresT))
            hp = half // PARTS_P

            def terms(i, pT):
                a = rounded(lax.dynamic_slice_in_dim(Wo, i * hp, hp, 0), duo)
                b = rounded(lax.dynamic_slice_in_dim(W, side * half + i * hp, hp, 0), dup)
                return lax.dynamic_update_slice_in_dim(pT, a + b, i * hp, 0)

            pT = lax.fori_loop(0, PARTS_P, terms, jnp.zeros((half, nt), f32))
            pT = plain(pT)
            dnT = plain(lax.psum_scatter(pT, "tp", scatter_dimension=0, axis_index_groups=rows, tiled=True))
            return pT, dnT, dresT

        pT, dnT, dresT = first(W, dup, dres)
        over = lax.pmax(over.astype(i32), "dp")

        q = jnp.where(trank < ROWS, (idp // vs) * ROWS + trank, -1)
        oh = (iota((nt, ntp * ROWS), 1) == q[:, None]).astype(bf16)
        rsg = lax.map(lambda v: norm(v)[0], xg.reshape(PARTS_R, -1, d)).reshape(-1, 1)
        rst = lax.map(
            lambda v: jnp.sum(jnp.where(iota((ntp * ROWS, v.shape[0]), 0) == v[None, :], rsg, 0.0), axis=0),
            q.reshape(PARTS_R, -1),
        ).reshape(nt)
        step = d // PARTS

        def chunk(i, c):
            xT, u, dW = c
            xc = lax.dynamic_slice_in_dim(xg, i * step, step, 1)
            xc = lax.dot_general(xc, oh, (((0,), (1,)), ((), ())), preferred_element_type=f32).astype(bf16)
            gc = lax.dynamic_slice_in_dim(gf, i * step, step, 0)
            nc = (xc.astype(f32) * rst[None, :] * gc[:, None]).astype(bf16)
            u = u + dot(nc, lax.dynamic_slice_in_dim(W, i * step, step, 0), c0)
            dW = lax.dynamic_update_slice_in_dim(dW, dot(nc, dup), i * step, 0)
            return lax.dynamic_update_slice_in_dim(xT, xc, i * step, 0), u, dW

        xT = jnp.zeros((d, nt), bf16)
        xT, u, dW = lax.fori_loop(0, PARTS, chunk, (xT, jnp.zeros((nt, W.shape[1]), f32), jnp.zeros(W.shape, f32)))
        xT = plain(xT)
        un = u.astype(bf16).reshape(ntp, nk, ts, -1).transpose(1, 0, 2, 3).reshape(nk, t, -1)
        xo = lax.optimization_barrier(plain(lax.dynamic_slice_in_dim(xT, me * own, own, 1))).T

        def ahead(xT, rst, pT):
            hp = half // PARTS_P

            def part(i, c):
                mp, dgp = c
                at = side * half + i * hp
                nh = lax.dynamic_slice_in_dim(xT, at, hp, 0).astype(f32) * rst[None, :]
                gh = lax.dynamic_slice_in_dim(gf, at, hp, 0)
                term = nh * lax.dynamic_slice_in_dim(pT, i * hp, hp, 0)
                mp = mp + jnp.sum(term * gh[:, None], axis=0)
                return mp, lax.dynamic_update_slice_in_dim(dgp, jnp.sum(term, axis=1), i * hp, 0)

            mp, dgp = lax.fori_loop(0, PARTS_P, part, (jnp.zeros((nt,), f32), jnp.zeros((half,), f32)))
            dgp = jnp.concatenate([jnp.where(side == 0, dgp, 0.0), jnp.where(side == 1, dgp, 0.0)])
            both = lax.psum(jnp.concatenate([mp, dgp]), "tp")
            return both[:nt] * (1.0 / d), both[nt:]

        def behind(xT, rst, m, dnT, dresT):
            nh = lax.dynamic_slice_in_dim(xT, start, dc, 0).astype(f32) * rst[None, :]
            gdn = lax.dynamic_slice_in_dim(gf, start, dc, 0)[:, None] * dnT
            dx = dresT.astype(f32) + rst[None, :] * (gdn - nh * m[None, :])
            return dx.astype(bf16)

        def columns(v):
            return v.reshape(npair, 2, -1, dc).transpose(2, 1, 0, 3).reshape(-1, d)

        m, dg = ahead(xT, rst, pT)
        dnT, m, dg, un, dW, xo, over = lax.optimization_barrier((dnT, m, dg, un, dW, xo, over))
        dxT = behind(xT, rst, m, dnT, dresT)
        dxT = lax.optimization_barrier(dxT)
        dEc = lax.dot_general(oh, dxT, (((0,), (1,)), ((), ())), preferred_element_type=f32)
        got = lax.all_to_all(dEc.reshape(ntp, ROWS, dc), "tp", 0, 0, tiled=True)
        put = (iota((vs, ROWS), 1) == mrank[:, None]).astype(f32)
        dE = jnp.dot(put, columns(got), precision=lax.Precision.HIGHEST, preferred_element_type=f32)
        outs = (over, un, xo.reshape(nk, ts, d), dE, dW, dg)

        def slow(c):
            def micro(k, c):
                us, xs, dE, dW, dg = c
                duk = lax.dynamic_index_in_dim(du, k, 0, False)
                idk = lax.dynamic_index_in_dim(ids, k, 0, False)
                oht = (iota((vs, t), 0) == (idk - lo)[None, :]).astype(bf16)
                x = lax.psum(dot(oht, E, c0).astype(bf16), "tp")
                rs, nh = norm(x)
                nk_ = (nh * gf).astype(bf16)
                u = dot(nk_, W).astype(bf16)
                part = lax.dynamic_slice_in_dim(x, me * ts, ts, 0)
                pk = dot(duk, W, c1).astype(bf16)
                dn = jnp.sum(lax.all_to_all(pk.reshape(ntp, ts, d), "tp", 0, 0, tiled=True).astype(f32), axis=0)
                rs, nh = norm(part)
                gdn = gf * dn
                dr = lax.dynamic_index_in_dim(dres, k, 0, False).astype(f32)
                dx = dr + rs * (gdn - nh * jnp.mean(nh * gdn, axis=-1, keepdims=True))
                dxa = lax.all_gather(dx.astype(bf16), "tp", axis=0, tiled=True)
                us = lax.dynamic_update_index_in_dim(us, u, k, 0)
                xs = lax.dynamic_update_index_in_dim(xs, part, k, 0)
                return us, xs, dE + dot(oht, dxa), dW + dot(nk_, duk, c0), dg + jnp.sum(dn * nh, axis=0)

            us, xs, dE, dW, dg = c[1:]
            c = lax.fori_loop(0, nk, micro, (us, xs, jnp.zeros_like(dE), jnp.zeros_like(dW), jnp.zeros_like(dg)))
            return (jnp.int32(0),) + c[:4] + (lax.psum(c[4], "tp"),)

        return lax.while_loop(lambda c: c[0] > 0, slow, outs)[1:]

    return jax.shard_map(
        body,
        mesh=mesh,
        in_specs=(P("dp", None), P("tp", None), P(None), P(None, "tp"), P("dp", None, "tp"), P("dp", "tp", None)),
        out_specs=(P("dp", None, "tp"), P("dp", "tp", None), P(("dp", "tp"), None), P("dp", "tp"), P("dp")),
        check_vma=False,
    )
```

```python
import functools

import jax
import jax.numpy as jnp
from jax import lax
from jax.experimental import pallas as pl
from jax.experimental.pallas import tpu as pltpu
from jax.sharding import PartitionSpec as P

EPS = 1e-6
ROWS = 64
LOW = 64


def hand_out(n, q_ref, dx_ref, out_ref, buf, send_sem, recv_sem, own_sem):
    me = lax.axis_index("tp")
    place = (me % 2) * (n // 2) + me // 2
    rows = buf.shape[1]
    barrier = pltpu.get_barrier_semaphore()

    def greet(k, _):
        pl.semaphore_signal(barrier, inc=1, device_id={"tp": lax.rem(me + k, n)}, device_id_type=pl.DeviceIdType.MESH)
        return 0

    lax.fori_loop(1, n, greet, 0)

    def sums(k):
        owner = lax.rem(me + k, n)
        slot = lax.broadcasted_iota(jnp.int32, (rows, q_ref.shape[1]), 0) + owner * rows
        oh = (slot == q_ref[...]).astype(jnp.float32).astype(jnp.bfloat16)
        buf[k] = lax.dot_general(oh, dx_ref[...], (((1,), (1,)), ((), ())), preferred_element_type=jnp.float32)

    def offset(j):
        return n // 2 + (2 * (j % 2) - 1) * ((j + 1) // 2) * -1

    def copy(k):
        return pltpu.make_async_remote_copy(
            src_ref=buf.at[k],
            dst_ref=out_ref.at[place],
            send_sem=send_sem.at[k],
            recv_sem=recv_sem.at[k],
            device_id={"tp": lax.rem(me + k, n)},
            device_id_type=pl.DeviceIdType.MESH,
        )

    sums(offset(0))
    pl.semaphore_wait(barrier, n - 1)

    def step(j, _):
        sums(offset(j + 1))
        copy(offset(j)).start()
        return 0

    lax.fori_loop(0, n - 2, step, 0)
    sums(0)
    copy(offset(n - 2)).start()
    mine = pltpu.make_async_copy(buf.at[0], out_ref.at[place], own_sem)
    mine.start()

    def finish(k, _):
        copy(k).wait()
        return 0

    lax.fori_loop(1, n, finish, 0)
    mine.wait()


def solution(mesh):
    ntp = mesh.shape["tp"]

    def body(ids, E, g, W, du, dres):
        f32, bf16, i32 = jnp.float32, jnp.bfloat16, jnp.int32
        vs, d = E.shape
        nk, t = ids.shape
        ts = t // ntp
        nt = nk * t
        own = nk * ts
        hn = ntp * vs // LOW
        hs = vs // LOW
        me = lax.axis_index("tp")
        lo = me * vs
        gf = g.astype(f32)
        c0 = (((0,), (0,)), ((), ()))
        c1 = (((1,), (1,)), ((), ()))

        def dot(a, b, c=(((1,), (0,)), ((), ()))):
            return lax.dot_general(a, b, c, preferred_element_type=f32)

        def iota(shape, dim):
            return lax.broadcasted_iota(i32, shape, dim)

        def norm(v):
            vf = v.astype(f32)
            rs = lax.rsqrt(jnp.mean(vf * vf, axis=-1, keepdims=True) + EPS)
            return rs, vf * rs

        idp = ids.reshape(nk, ntp, ts).transpose(1, 0, 2).reshape(nt)
        dup = du.reshape(nk, ntp, ts, -1).transpose(1, 0, 2, 3).reshape(nt, -1)

        isl = iota((LOW, nt), 0) == (idp % LOW)[None, :]
        ish = iota((hn, nt), 0) == (idp // LOW)[None, :]
        pres = dot(ish.astype(bf16), isl.astype(bf16), c1) > 0
        upper = (iota((LOW, LOW), 0) < iota((LOW, LOW), 1)).astype(bf16)
        inrow = dot(pres.astype(bf16), upper)
        tot = jnp.sum(pres.astype(f32), axis=1)
        ha, hb = iota((hn, hn), 0), iota((hn, hn), 1)
        off = jnp.sum(jnp.where((ha // hs == hb // hs) & (hb < ha), tot[None, :], 0.0), axis=1)
        rank = jnp.where(pres, inrow + off[:, None], -1.0)
        over = jnp.max(rank) >= ROWS
        trank = dot(inrow.astype(bf16), isl.astype(bf16)) + off[:, None]
        trank = jnp.sum(jnp.where(ish, trank, 0.0), axis=0).astype(i32)
        mrank = lax.dynamic_slice_in_dim(rank, me * hs, hs, 0).reshape(vs).astype(i32)

        sel = (iota((ROWS, vs), 0) == mrank[None, :]).astype(bf16)
        xg = lax.all_gather(dot(sel, E).astype(bf16), "tp", axis=0, tiled=True)

        half, dc, npair = d // 2, d // ntp, ntp // 2
        side = me % 2
        swap = [(i, i ^ 1) for i in range(ntp)]
        rows = [list(range(c, ntp, 2)) for c in range(2)]
        start = side * half + (me // 2) * dc

        def rounded(a, b):
            return lax.reduce_precision(dot(a, b, c1), 8, 7)

        def first(W, dup, dres):
            Wo = lax.ppermute(lax.dynamic_slice_in_dim(W, (1 - side) * half, half, 0), "tp", swap)
            duo = lax.ppermute(dup, "tp", swap)
            dr = dres.reshape(own, 2, npair, dc).transpose(0, 2, 1, 3).reshape(own, d)
            dresT = lax.all_to_all(dr, "tp", 1, 0, tiled=True).T
            dup, duo, Wo, dresT = lax.optimization_barrier((dup, duo, Wo, dresT))
            pT = rounded(Wo, duo) + rounded(lax.dynamic_slice_in_dim(W, side * half, half, 0), dup)
            pT = lax.optimization_barrier(pT)
            dnT = lax.psum_scatter(pT, "tp", scatter_dimension=0, axis_index_groups=rows, tiled=True)
            return pT, dnT, dresT

        pT, dnT, dresT = first(W, dup, dres)
        over = lax.pmax(over.astype(i32), "dp")

        q = jnp.where(trank < ROWS, (idp // vs) * ROWS + trank, -1)
        oh = (iota((nt, ntp * ROWS), 1) == q[:, None]).astype(bf16)
        ohT = iota((ntp * ROWS, nt), 0) == q[None, :]
        rst = jnp.sum(jnp.where(ohT, norm(xg)[0], 0.0), axis=0)
        xT = lax.dot_general(xg, oh, (((0,), (1,)), ((), ())), preferred_element_type=f32).astype(bf16)
        qo = lax.dynamic_slice_in_dim(q, me * own, own, 0)
        oho = (iota((own, ntp * ROWS), 1) == qo[:, None]).astype(bf16)
        xo = dot(oho, xg).astype(bf16)

        def ahead(xT, rst, pT, W, dup):
            nh = lax.dynamic_slice_in_dim(xT, side * half, half, 0).astype(f32) * rst[None, :]
            gh = lax.dynamic_slice_in_dim(gf, side * half, half, 0)
            mp = jnp.sum(nh * gh[:, None] * pT, axis=0)
            dgp = jnp.sum(nh * pT, axis=1)
            dgp = jnp.concatenate([jnp.where(side == 0, dgp, 0.0), jnp.where(side == 1, dgp, 0.0)])
            nT = (xT.astype(f32) * rst[None, :] * gf[:, None]).astype(bf16)
            u = dot(nT, W, c0).astype(bf16)
            dW = dot(nT, dup)
            un = u.reshape(ntp, nk, ts, -1).transpose(1, 0, 2, 3).reshape(nk, t, -1)
            both = lax.psum(jnp.concatenate([mp, dgp]), "tp")
            return both[:nt] * (1.0 / d), both[nt:], un, dW

        def behind(xT, rst, m, dnT, dresT):
            nh = lax.dynamic_slice_in_dim(xT, start, dc, 0).astype(f32) * rst[None, :]
            gdn = lax.dynamic_slice_in_dim(gf, start, dc, 0)[:, None] * dnT
            dx = dresT.astype(f32) + rst[None, :] * (gdn - nh * m[None, :])
            return dx.astype(bf16)

        m, dg, un, dW = ahead(xT, rst, pT, W, dup)
        dnT, m, dg, un, dW, xo, over = lax.optimization_barrier((dnT, m, dg, un, dW, xo, over))
        dxT = behind(xT, rst, m, dnT, dresT)
        got = pl.pallas_call(
            functools.partial(hand_out, ntp),
            out_shape=jax.ShapeDtypeStruct((ntp, ROWS, dc), f32),
            in_specs=[pl.BlockSpec(memory_space=pltpu.VMEM)] * 2,
            out_specs=pl.BlockSpec(memory_space=pl.ANY),
            scratch_shapes=[
                pltpu.VMEM((ntp, ROWS, dc), f32),
                pltpu.SemaphoreType.DMA((ntp,)),
                pltpu.SemaphoreType.DMA((ntp,)),
                pltpu.SemaphoreType.DMA,
            ],
            compiler_params=pltpu.CompilerParams(collective_id=0, has_side_effects=True),
        )(q.reshape(1, nt), dxT)
        put = (iota((vs, ROWS), 1) == mrank[:, None]).astype(f32)
        dE = jnp.dot(put, got.transpose(1, 0, 2).reshape(ROWS, d), precision=lax.Precision.HIGHEST, preferred_element_type=f32)
        outs = (over, un, xo.reshape(nk, ts, d), dE, dW, dg)

        def slow(c):
            def micro(k, c):
                us, xs, dE, dW, dg = c
                duk = lax.dynamic_index_in_dim(du, k, 0, False)
                idk = lax.dynamic_index_in_dim(ids, k, 0, False)
                oht = (iota((vs, t), 0) == (idk - lo)[None, :]).astype(bf16)
                x = lax.psum(dot(oht, E, c0).astype(bf16), "tp")
                rs, nh = norm(x)
                nk_ = (nh * gf).astype(bf16)
                u = dot(nk_, W).astype(bf16)
                part = lax.dynamic_slice_in_dim(x, me * ts, ts, 0)
                pk = dot(duk, W, c1).astype(bf16)
                dn = jnp.sum(lax.all_to_all(pk.reshape(ntp, ts, d), "tp", 0, 0, tiled=True).astype(f32), axis=0)
                rs, nh = norm(part)
                gdn = gf * dn
                dr = lax.dynamic_index_in_dim(dres, k, 0, False).astype(f32)
                dx = dr + rs * (gdn - nh * jnp.mean(nh * gdn, axis=-1, keepdims=True))
                dxa = lax.all_gather(dx.astype(bf16), "tp", axis=0, tiled=True)
                us = lax.dynamic_update_index_in_dim(us, u, k, 0)
                xs = lax.dynamic_update_index_in_dim(xs, part, k, 0)
                return us, xs, dE + dot(oht, dxa), dW + dot(nk_, duk, c0), dg + jnp.sum(dn * nh, axis=0)

            us, xs, dE, dW, dg = c[1:]
            c = lax.fori_loop(0, nk, micro, (us, xs, jnp.zeros_like(dE), jnp.zeros_like(dW), jnp.zeros_like(dg)))
            return (jnp.int32(0),) + c[:4] + (lax.psum(c[4], "tp"),)

        return lax.while_loop(lambda c: c[0] > 0, slow, outs)[1:]

    return jax.shard_map(
        body,
        mesh=mesh,
        in_specs=(P("dp", None), P("tp", None), P(None), P(None, "tp"), P("dp", None, "tp"), P("dp", "tp", None)),
        out_specs=(P("dp", None, "tp"), P("dp", "tp", None), P(("dp", "tp"), None), P("dp", "tp"), P("dp")),
        check_vma=False,
    )
```

```python
import functools

import jax
import jax.numpy as jnp
from jax import lax
from jax.experimental import pallas as pl
from jax.experimental.pallas import tpu as pltpu
from jax.sharding import PartitionSpec as P

EPS = 1e-6
ROWS = 56
LOW = 64


def hand_out(n, q_ref, dx_ref, out_ref, buf, send_sem, recv_sem, own_sem):
    me = lax.axis_index("tp")
    place = (me % 2) * (n // 2) + me // 2
    rows = buf.shape[1]
    barrier = pltpu.get_barrier_semaphore()

    def greet(k, _):
        pl.semaphore_signal(barrier, inc=1, device_id={"tp": lax.rem(me + k, n)}, device_id_type=pl.DeviceIdType.MESH)
        return 0

    lax.fori_loop(1, n, greet, 0)

    def sums(k):
        owner = lax.rem(me + k, n)
        slot = lax.broadcasted_iota(jnp.int32, (rows, q_ref.shape[1]), 0) + owner * rows
        oh = (slot == q_ref[...]).astype(jnp.float32).astype(jnp.bfloat16)
        buf[k] = lax.dot_general(oh, dx_ref[...], (((1,), (1,)), ((), ())), preferred_element_type=jnp.float32)

    def offset(j):
        return n // 2 + (2 * (j % 2) - 1) * ((j + 1) // 2) * -1

    def copy(k):
        return pltpu.make_async_remote_copy(
            src_ref=buf.at[k],
            dst_ref=out_ref.at[place],
            send_sem=send_sem.at[k],
            recv_sem=recv_sem.at[k],
            device_id={"tp": lax.rem(me + k, n)},
            device_id_type=pl.DeviceIdType.MESH,
        )

    sums(offset(0))
    pl.semaphore_wait(barrier, n - 1)

    def step(j, _):
        sums(offset(j + 1))
        copy(offset(j)).start()
        return 0

    lax.fori_loop(0, n - 2, step, 0)
    sums(0)
    copy(offset(n - 2)).start()
    mine = pltpu.make_async_copy(buf.at[0], out_ref.at[place], own_sem)
    mine.start()

    def finish(k, _):
        copy(k).wait()
        return 0

    lax.fori_loop(1, n, finish, 0)
    mine.wait()


def solution(mesh):
    ntp = mesh.shape["tp"]

    def body(ids, E, g, W, du, dres):
        f32, bf16, i32 = jnp.float32, jnp.bfloat16, jnp.int32
        vs, d = E.shape
        nk, t = ids.shape
        ts = t // ntp
        nt = nk * t
        own = nk * ts
        hn = ntp * vs // LOW
        hs = vs // LOW
        me = lax.axis_index("tp")
        lo = me * vs
        gf = g.astype(f32)
        c0 = (((0,), (0,)), ((), ()))
        c1 = (((1,), (1,)), ((), ()))

        def dot(a, b, c=(((1,), (0,)), ((), ()))):
            return lax.dot_general(a, b, c, preferred_element_type=f32)

        def iota(shape, dim):
            return lax.broadcasted_iota(i32, shape, dim)

        def norm(v):
            vf = v.astype(f32)
            rs = lax.rsqrt(jnp.mean(vf * vf, axis=-1, keepdims=True) + EPS)
            return rs, vf * rs

        idp = ids.reshape(nk, ntp, ts).transpose(1, 0, 2).reshape(nt)
        dup = du.reshape(nk, ntp, ts, -1).transpose(1, 0, 2, 3).reshape(nt, -1)

        isl = iota((LOW, nt), 0) == (idp % LOW)[None, :]
        ish = iota((hn, nt), 0) == (idp // LOW)[None, :]
        pres = dot(ish.astype(bf16), isl.astype(bf16), c1) > 0
        upper = (iota((LOW, LOW), 0) < iota((LOW, LOW), 1)).astype(bf16)
        inrow = dot(pres.astype(bf16), upper)
        tot = jnp.sum(pres.astype(f32), axis=1)
        ha, hb = iota((hn, hn), 0), iota((hn, hn), 1)
        off = jnp.sum(jnp.where((ha // hs == hb // hs) & (hb < ha), tot[None, :], 0.0), axis=1)
        rank = jnp.where(pres, inrow + off[:, None], -1.0)
        over = jnp.max(rank) >= ROWS
        trank = dot(inrow.astype(bf16), isl.astype(bf16)) + off[:, None]
        trank = jnp.sum(jnp.where(ish, trank, 0.0), axis=0).astype(i32)
        mrank = lax.dynamic_slice_in_dim(rank, me * hs, hs, 0).reshape(vs).astype(i32)

        sel = (iota((ROWS, vs), 0) == mrank[None, :]).astype(bf16)
        xg = lax.all_gather(dot(sel, E).astype(bf16), "tp", axis=0, tiled=True)

        half, dc, npair = d // 2, d // ntp, ntp // 2
        side = me % 2
        swap = [(i, i ^ 1) for i in range(ntp)]
        rows = [list(range(c, ntp, 2)) for c in range(2)]
        start = side * half + (me // 2) * dc

        def rounded(a, b):
            return lax.reduce_precision(dot(a, b, c1), 8, 7)

        def first(W, dup, dres):
            Wo = lax.ppermute(lax.dynamic_slice_in_dim(W, (1 - side) * half, half, 0), "tp", swap)
            duo = lax.ppermute(dup, "tp", swap)
            dr = dres.reshape(own, 2, npair, dc).transpose(0, 2, 1, 3).reshape(own, d)
            dresT = lax.all_to_all(dr, "tp", 1, 0, tiled=True).T
            dup, duo, Wo, dresT = lax.optimization_barrier((dup, duo, Wo, dresT))
            pT = rounded(Wo, duo) + rounded(lax.dynamic_slice_in_dim(W, side * half, half, 0), dup)
            pT = lax.optimization_barrier(pT)
            dnT = lax.psum_scatter(pT, "tp", scatter_dimension=0, axis_index_groups=rows, tiled=True)
            return pT, dnT, dresT

        pT, dnT, dresT = first(W, dup, dres)
        over = lax.pmax(over.astype(i32), "dp")

        q = jnp.where(trank < ROWS, (idp // vs) * ROWS + trank, -1)
        oh = (iota((nt, ntp * ROWS), 1) == q[:, None]).astype(bf16)
        ohT = iota((ntp * ROWS, nt), 0) == q[None, :]
        rst = jnp.sum(jnp.where(ohT, norm(xg)[0], 0.0), axis=0)
        xT = lax.dot_general(xg, oh, (((0,), (1,)), ((), ())), preferred_element_type=f32).astype(bf16)
        qo = lax.dynamic_slice_in_dim(q, me * own, own, 0)
        oho = (iota((own, ntp * ROWS), 1) == qo[:, None]).astype(bf16)
        xo = dot(oho, xg).astype(bf16)

        def ahead(xT, rst, pT, W, dup):
            nh = lax.dynamic_slice_in_dim(xT, side * half, half, 0).astype(f32) * rst[None, :]
            gh = lax.dynamic_slice_in_dim(gf, side * half, half, 0)
            mp = jnp.sum(nh * gh[:, None] * pT, axis=0)
            dgp = jnp.sum(nh * pT, axis=1)
            dgp = jnp.concatenate([jnp.where(side == 0, dgp, 0.0), jnp.where(side == 1, dgp, 0.0)])
            nT = (xT.astype(f32) * rst[None, :] * gf[:, None]).astype(bf16)
            u = dot(nT, W, c0).astype(bf16)
            dW = dot(nT, dup)
            un = u.reshape(ntp, nk, ts, -1).transpose(1, 0, 2, 3).reshape(nk, t, -1)
            both = lax.psum(jnp.concatenate([mp, dgp]), "tp")
            return both[:nt] * (1.0 / d), both[nt:], un, dW

        def behind(xT, rst, m, dnT, dresT):
            nh = lax.dynamic_slice_in_dim(xT, start, dc, 0).astype(f32) * rst[None, :]
            gdn = lax.dynamic_slice_in_dim(gf, start, dc, 0)[:, None] * dnT
            dx = dresT.astype(f32) + rst[None, :] * (gdn - nh * m[None, :])
            return dx.astype(bf16)

        m, dg, un, dW = ahead(xT, rst, pT, W, dup)
        dnT, m, dg, un, dW, xo, over = lax.optimization_barrier((dnT, m, dg, un, dW, xo, over))
        dxT = behind(xT, rst, m, dnT, dresT)
        got = pl.pallas_call(
            functools.partial(hand_out, ntp),
            out_shape=jax.ShapeDtypeStruct((ntp, ROWS, dc), f32),
            in_specs=[pl.BlockSpec(memory_space=pltpu.VMEM)] * 2,
            out_specs=pl.BlockSpec(memory_space=pl.ANY),
            scratch_shapes=[
                pltpu.VMEM((ntp, ROWS, dc), f32),
                pltpu.SemaphoreType.DMA((ntp,)),
                pltpu.SemaphoreType.DMA((ntp,)),
                pltpu.SemaphoreType.DMA,
            ],
            compiler_params=pltpu.CompilerParams(collective_id=0, has_side_effects=True),
        )(q.reshape(1, nt), dxT)
        put = (iota((vs, ROWS), 1) == mrank[:, None]).astype(f32)
        dE = jnp.dot(put, got.transpose(1, 0, 2).reshape(ROWS, d), precision=lax.Precision.HIGHEST, preferred_element_type=f32)
        outs = (over, un, xo.reshape(nk, ts, d), dE, dW, dg)

        def slow(c):
            def micro(k, c):
                us, xs, dE, dW, dg = c
                duk = lax.dynamic_index_in_dim(du, k, 0, False)
                idk = lax.dynamic_index_in_dim(ids, k, 0, False)
                oht = (iota((vs, t), 0) == (idk - lo)[None, :]).astype(bf16)
                x = lax.psum(dot(oht, E, c0).astype(bf16), "tp")
                rs, nh = norm(x)
                nk_ = (nh * gf).astype(bf16)
                u = dot(nk_, W).astype(bf16)
                part = lax.dynamic_slice_in_dim(x, me * ts, ts, 0)
                pk = dot(duk, W, c1).astype(bf16)
                dn = jnp.sum(lax.all_to_all(pk.reshape(ntp, ts, d), "tp", 0, 0, tiled=True).astype(f32), axis=0)
                rs, nh = norm(part)
                gdn = gf * dn
                dr = lax.dynamic_index_in_dim(dres, k, 0, False).astype(f32)
                dx = dr + rs * (gdn - nh * jnp.mean(nh * gdn, axis=-1, keepdims=True))
                dxa = lax.all_gather(dx.astype(bf16), "tp", axis=0, tiled=True)
                us = lax.dynamic_update_index_in_dim(us, u, k, 0)
                xs = lax.dynamic_update_index_in_dim(xs, part, k, 0)
                return us, xs, dE + dot(oht, dxa), dW + dot(nk_, duk, c0), dg + jnp.sum(dn * nh, axis=0)

            us, xs, dE, dW, dg = c[1:]
            c = lax.fori_loop(0, nk, micro, (us, xs, jnp.zeros_like(dE), jnp.zeros_like(dW), jnp.zeros_like(dg)))
            return (jnp.int32(0),) + c[:4] + (lax.psum(c[4], "tp"),)

        return lax.while_loop(lambda c: c[0] > 0, slow, outs)[1:]

    return jax.shard_map(
        body,
        mesh=mesh,
        in_specs=(P("dp", None), P("tp", None), P(None), P(None, "tp"), P("dp", None, "tp"), P("dp", "tp", None)),
        out_specs=(P("dp", None, "tp"), P("dp", "tp", None), P(("dp", "tp"), None), P("dp", "tp"), P("dp")),
        check_vma=False,
    )
```
